32 devices in a mesh: owner: 16 (over z, y, core), rows: 2 (over x).
Axes of the slice: x: 2, y: 2, z: 4, core: 2. Of those that a mesh axis runs over, the one named last changes fastest.
Arguments:
- w_gate: float32 [64, 2048, 1024], P('owner', 'rows'), may hold values from -0.1875 to 0.1875
- avg_gate: float32 [64, 2048, 1024], P('owner', 'rows'), may hold values from -0.125 to 0.125
- w_up: float32 [64, 2048, 1024], P('owner', 'rows'), may hold values from -0.1875 to 0.1875
- avg_up: float32 [64, 2048, 1024], P('owner', 'rows'), may hold values from -0.125 to 0.125
- mix_share: float32 [64], P('owner'), may hold values from 0.2 to 0.8
- router_weight: float32 [2048, 64], P('rows', 'owner'), may hold values from -0.125 to 0.125
- router_gain: float32 [2048], P('rows'), may hold values from 0.25 to 1.75
Outputs:
- serve_gate: bfloat16 [64, 2048, 1024], P('owner')
- serve_up: bfloat16 [64, 2048, 1024], P('owner')
- scale_gate: float32 [64, 1024], P('owner')
- scale_up: float32 [64, 1024], P('owner')
- serve_router: bfloat16 [2048, 64], replicated
The draws below stay inside these ranges and needn't reach their ends.
All inputs are finite; a program needn't handle non-finite values.
Results may differ from the reference program's by a relative error of at most 0.0015.
Values may be sent and summed in bfloat16 or wider, within the bound.
No kernel may reach another device: no remote copies, remote signals or barrier semaphores. Data moves between devices by JAX's collectives and lax.ppermute only.
A program may use at most 192 MiB of HBM per device.

```python
import jax
import jax.numpy as jnp
from jax import lax

EXPERTS = 64
D_MODEL = 2048
D_EXPERT = 1024


def raised(drawn, own_key, source, target, blocks, factor):
    def block_of(axis_at):
        return (jnp.arange(drawn.shape[axis_at]) // (drawn.shape[axis_at] // blocks)).reshape((-1,) + (1,) * (drawn.ndim - 1 - axis_at))

    near = jax.random.permutation(own_key, blocks)[block_of(target)]
    far = (block_of(target) + blocks // 2) % blocks
    return jnp.where((block_of(source) == near) | (block_of(source) == far), factor * drawn, drawn)


def level_of(key, shape, pieces, least, largest):
    factor_of = 1.0
    for position, blocks in pieces:
        heights = jax.random.uniform(jax.random.fold_in(jax.random.fold_in(key, 6), position), (blocks,), jnp.float32, least / len(pieces), largest / len(pieces))
        factor_of = factor_of * jnp.repeat(jnp.exp(heights), shape[position] // blocks).reshape((-1,) + (1,) * (len(shape) - 1 - position))
    return factor_of


def scatter_about(key, dims, width, most, cuts=(), held_as=jnp.bfloat16):
    drawn = jax.random.normal(key, dims, jnp.float32) * width
    if len(cuts) > 0:
        drawn = level_of(key, dims, cuts, -0.22, 0.18) * drawn
    return jnp.clip(drawn, min=-most, max=most).astype(held_as)


def heavy_noise(own_key, shape, spread, reach, split, heavy, kind=jnp.bfloat16):
    values = spread * jax.random.normal(own_key, shape, jnp.float32)
    if split:
        values = values * level_of(own_key, shape, split, -0.22, 0.18)
    return jnp.clip(raised(values, jax.random.fold_in(own_key, 3), *heavy), -reach, reach).astype(kind)


def setup_inputs(seed: int = 0) -> dict:
    key_of = jax.random.split(jax.random.key(seed), 8)
    w_gate = heavy_noise(key_of[0], (EXPERTS, D_MODEL, D_EXPERT), D_MODEL ** -0.5, 0.1875, ((0, 16), (1, 2)), (1, 2, 2, 2.0), jnp.float32)
    avg_gate = scatter_about(key_of[1], (EXPERTS, D_MODEL, D_EXPERT), D_MODEL ** -0.5, 0.125, ((0, 16), (1, 2)), jnp.float32)
    w_up = heavy_noise(key_of[2], (EXPERTS, D_MODEL, D_EXPERT), D_MODEL ** -0.5, 0.1875, ((0, 16), (1, 2)), (1, 2, 2, 2.0), jnp.float32)
    avg_up = scatter_about(key_of[3], (EXPERTS, D_MODEL, D_EXPERT), D_MODEL ** -0.5, 0.125, ((0, 16), (1, 2)), jnp.float32)
    mix_share = jnp.clip(0.2 + 0.6 * jax.random.uniform(key_of[4], (EXPERTS,), jnp.float32) ** level_of(key_of[4], (EXPERTS,), ((0, 16),), -0.2, 0.2), 0.2, 0.8)
    router_weight = scatter_about(key_of[5], (D_MODEL, EXPERTS), D_MODEL ** -0.5, 0.125, ((0, 2), (1, 16)), jnp.float32)
    router_gain = jnp.clip(1.0 + 0.15 * jax.random.normal(key_of[6], (D_MODEL,), jnp.float32), 0.25, 1.75)
    return {"w_gate": w_gate, "avg_gate": avg_gate, "w_up": w_up, "avg_up": avg_up, "mix_share": mix_share, "router_weight": router_weight, "router_gain": router_gain}


def reference(w_gate, avg_gate, w_up, avg_up, mix_share, router_weight, router_gain):
    fresh_gate = mix_share[:, None, None] * w_gate + (1.0 - mix_share[:, None, None]) * avg_gate
    fresh_up = mix_share[:, None, None] * w_up + (1.0 - mix_share[:, None, None]) * avg_up
    scale_gate = jnp.sqrt(lax.optimization_barrier(jnp.sum(fresh_gate * fresh_gate, axis=1)))
    serve_gate = (fresh_gate / jnp.expand_dims(scale_gate, 1)).astype(jnp.bfloat16)
    scale_up = jnp.sqrt(lax.optimization_barrier(jnp.sum(fresh_up * fresh_up, axis=1)))
    serve_up = (fresh_up / jnp.expand_dims(scale_up, 1)).astype(jnp.bfloat16)
    serve_router = (router_weight * router_gain[:, None]).astype(jnp.bfloat16)
    return (serve_gate, serve_up, scale_gate, scale_up, serve_router)
```

```python
import jax
import jax.numpy as jnp
from jax import lax
from jax.experimental import pallas as pl
from jax.experimental.pallas import tpu as pltpu
from jax.sharding import PartitionSpec as P


ANY = pl.BlockSpec(memory_space=pl.ANY)
SMALL = pl.BlockSpec(memory_space=pltpu.SMEM)


def block_rows(rows, most):
    block = min(rows, most)
    while rows % block:
        block -= 16
    return block


def column_sums(w, avg, mix, first, count, most, out, at, slots, after):
    _, rows, cols = w.shape
    block = block_rows(rows, most)
    steps = rows // block

    def kernel(mix_ref, w_ref, avg_ref, *rest):
        out_ref, acc = rest[-2], rest[-1]
        e, i = pl.program_id(0), pl.program_id(1)
        share = mix_ref[first + e]
        fresh = share * w_ref[0] + (1.0 - share) * avg_ref[0]
        part = jnp.sum((fresh * fresh).reshape(block // 8, 8, cols), axis=0)

        @pl.when(i == 0)
        def _():
            acc[...] = part

        @pl.when(i > 0)
        def _():
            acc[...] += part

        @pl.when(i == steps - 1)
        def _():
            out_ref[0] = jnp.sum(acc[...], axis=0, keepdims=True)

    spec = pl.BlockSpec((1, block, cols), lambda e, i: (first + e, i, 0))
    extra = ([] if out is None else [out]) + list(after)
    return pl.pallas_call(
        kernel,
        grid=(count, steps),
        in_specs=[SMALL, spec, spec] + [ANY] * len(extra),
        out_specs=pl.BlockSpec((1, 1, cols), lambda e, i: (at + e, 0, 0)),
        out_shape=jax.ShapeDtypeStruct((slots, 1, cols), jnp.float32),
        scratch_shapes=[pltpu.VMEM((8, cols), jnp.float32)],
        input_output_aliases={} if out is None else {3: 0},
    )(mix, w, avg, *extra)


def settle(w, avg, mix, parts, at, expert, start, count, most, place, out, whole_rows, after):
    experts, _, cols = w.shape
    block = block_rows(count, most)
    own = w.shape[1] // block

    def kernel(place_ref, mix_ref, w_ref, avg_ref, *rest):
        total = rest[0][0]
        for part_ref in rest[1 : len(parts)]:
            total = total + part_ref[0]
        send_ref, out_ref = rest[-2], rest[-1]
        share = mix_ref[expert]
        fresh = share * w_ref[0] + (1.0 - share) * avg_ref[0]
        inverse = 1.0 / jnp.sqrt(total)
        done = (fresh * inverse).astype(jnp.bfloat16)
        send_ref[0] = done
        out_ref[0] = done

    spec = pl.BlockSpec((1, block, cols), lambda i, p: (expert, start // block + i, 0))
    extra = ([] if out is None else [out]) + list(after)
    return pl.pallas_call(
        kernel,
        grid_spec=pltpu.PrefetchScalarGridSpec(
            num_scalar_prefetch=1,
            grid=(count // block,),
            in_specs=[SMALL, spec, spec]
            + [pl.BlockSpec((1, 1, cols), lambda i, p: (at, 0, 0))] * len(parts)
            + [ANY] * len(extra),
            out_specs=[
                pl.BlockSpec((1, block, cols), lambda i, p: (0, i, 0)),
                pl.BlockSpec((1, block, cols), lambda i, p: (expert, p[0] * own + start // block + i, 0)),
            ],
        ),
        out_shape=[
            pltpu.HBM((1, count, cols), jnp.bfloat16),
            pltpu.HBM((experts, whole_rows, cols), jnp.bfloat16),
        ],
        input_output_aliases={} if out is None else {4 + len(parts): 1},
    )(place, mix, w, avg, *parts, *extra)


def put(piece, source, out, expert, start, rows, most, after):
    _, count, cols = piece.shape
    block = block_rows(count, most)
    own = rows // block

    def kernel(source_ref, piece_ref, *rest):
        rest[-1][...] = piece_ref[...]

    return pl.pallas_call(
        kernel,
        grid_spec=pltpu.PrefetchScalarGridSpec(
            num_scalar_prefetch=1,
            grid=(count // block,),
            in_specs=[pl.BlockSpec((1, block, cols), lambda i, s: (0, i, 0))] + [ANY] * (1 + len(after)),
            out_specs=pl.BlockSpec((1, block, cols), lambda i, s: (expert, s[0] * own + start // block + i, 0)),
        ),
        out_shape=pltpu.HBM(out.shape, out.dtype),
        input_output_aliases={2: 0},
    )(source, piece, out, *after)


def plan(experts, rows):
    half = rows // 2
    pieces = [(0, 0, 0, half), (0, 0, half, half)]
    pieces += [(0, e, 0, rows) for e in range(1, experts)]
    pieces += [(1, e, 0, rows) for e in range(experts - 1)]
    last = (1, experts - 1)
    pieces += [(*last, 0, half), (*last, half, half // 2)]
    pieces += [(*last, half + half // 2, half // 4), (*last, half + half // 2 + half // 4, half // 4)]
    return pieces


def solution(mesh):
    ranks = mesh.shape["rows"]

    def moved(array, shift):
        return lax.ppermute(array, "rows", [(i, (i + shift) % ranks) for i in range(ranks)])

    def summands(part):
        if ranks == 2:
            return (part, moved(part, 1))
        return (jnp.sum(lax.all_gather(part, "rows"), axis=0),)

    def shards(w_gate, avg_gate, w_up, avg_up, mix_share, router_weight, router_gain):
        experts, rows, _ = w_gate.shape
        arrays = ((w_gate, avg_gate), (w_up, avg_up))
        here = lax.axis_index("rows").astype(jnp.int32).reshape(1)
        pieces = plan(experts, rows)
        outs = [None, None]
        sends = []

        part = column_sums(*arrays[0], mix_share, 0, 1, 128, None, 0, 1, ())
        first_parts = summands(part)

        def settled(k, after):
            which, expert, start, count = pieces[k]
            if which == 0 and expert == 0:
                parts, at = first_parts, 0
            else:
                parts, at = rest_parts, which * experts + expert - 1
            send, outs[which] = settle(
                *arrays[which], mix_share, parts, at, expert, start, count, 128 if k == 0 else 256,
                here, outs[which], rows * ranks, after,
            )
            sends.append(send)

        settled(0, ())
        part, slots = None, 2 * experts - 1
        if experts > 1:
            part = column_sums(*arrays[0], mix_share, 1, experts - 1, 256, None, 0, slots, (sends[0],))
        part = column_sums(*arrays[1], mix_share, 0, experts, 256, part, experts - 1, slots, (sends[0],))
        rest_parts = summands(part)

        gain, _ = lax.optimization_barrier((router_gain, part))
        part_router = (router_weight * gain[:, None]).astype(jnp.bfloat16).T
        if ranks == 2:
            other = moved(part_router, 1)
            first = here[0] == 0
            row_router = jnp.concatenate(
                [jnp.where(first, part_router, other), jnp.where(first, other, part_router)], axis=1
            )
        else:
            row_router = lax.all_gather(part_router, "rows", axis=1, tiled=True)

        for k in range(1, len(pieces)):
            settled(k, (sends[-1],) if k > 1 else (part,))

        row_router, _ = lax.optimization_barrier((row_router, sends[-1]))
        serve_router = lax.all_gather(row_router, "owner", axis=0, tiled=True).T

        after = (sends[-1],)
        for k, (which, expert, start, count) in enumerate(pieces):
            for shift in range(1, ranks):
                got = moved(sends[k], shift)
                source = (here + ranks - shift) % ranks
                outs[which] = put(got, source, outs[which], expert, start, rows, 512, after)
                after = (outs[0],) if which == 0 and pieces[(k + 1) % len(pieces)][0] == 1 else ()

        total = jnp.concatenate([sum(first_parts[1:], first_parts[0]), sum(rest_parts[1:], rest_parts[0])], axis=0)
        scales = jnp.sqrt(total[:, 0])
        scale_gate, scale_up = scales[:experts], scales[experts:]
        return (outs[0], outs[1], scale_gate, scale_up, serve_router)

    return jax.shard_map(
        shards,
        mesh=mesh,
        in_specs=(
            P("owner", "rows", None),
            P("owner", "rows", None),
            P("owner", "rows", None),
            P("owner", "rows", None),
            P("owner"),
            P("rows", "owner"),
            P("rows"),
        ),
        out_specs=(
            P("owner", None, None),
            P("owner", None, None),
            P("owner", None),
            P("owner", None),
            P(),
        ),
        check_vma=False,
    )
```
